256 devices in a mesh: grp: 32 (over x, z), node: 8 (over y, core).
Axes of the slice: x: 4, y: 4, z: 8, core: 2. Of those that a mesh axis runs over, the one named last changes fastest.
Arguments:
- initial: float32 [6, 32, 262144], P(None, None, ('grp', 'node')), may hold values from -0.5 to 16, as said below
- afferent_noise_level: float32 [32, 262144], P(None, ('grp', 'node')), may hold values from 0.12 to 0.32
- history: bfloat16 [64, 32, 262144], P(None, None, ('grp', 'node')), may hold values from 0 to 1
- weights: bfloat16 [256, 24, 128, 1024], P(('grp', 'node')), may hold values from -0.109375 to 0.109375
- lead_field: bfloat16 [128, 262144], P(None, ('grp', 'node')), may hold values from -0.0014648438 to 0.0014648438
- src_group: int32 [256, 24], replicated, may hold values from 0 to 31, as said below
- src_sub: int32 [256, 24], replicated, may hold values from 0 to 7
- delays: int32 [256, 24], replicated, may hold values from 6 to 63
- counts: int32 [256], replicated, may hold values from 16 to 24, as said below
Outputs:
- final_state: float32 [6, 32, 262144], P(None, None, ('grp', 'node'))
- sensors: float32 [6, 128, 32], replicated
The draws below stay inside these ranges and needn't reach their ends.
Inputs may be any that keep to these rules, and one draw needn't show every extreme that they name: `initial`: rows 0 to 2 are potentials and rows 3 to 5 their rates; row 0 lies within 0 and 0.4, row 1 within 4 and 16, row 2 within 0 and 8, rows 3 to 5 within -0.5 and 0.5. `src_group`: among the tiles k < counts[b] of a block b no owner group appears more than 1 times, and some block reaches 1. Tiles k >= counts[b] of block b are ignored; in every draw some block has 24 live tiles.
All inputs are finite; a program needn't handle non-finite values.
Results may differ from the reference program's by a relative error of at most 0.0003.
The reference program's roundings to bfloat16 on the way (of `cycle` and `potential`) count: a program that leaves them out, or rounds other values in their place, can miss the bound.
Values may be sent and summed in bfloat16 or wider, within the bound.
No kernel may reach another device: no remote copies, remote signals or barrier semaphores. Data moves between devices by JAX's collectives and lax.ppermute only.
A program may use at most 128 MiB of HBM per device.

```python
import math
import jax
import jax.numpy as jnp
from jax import lax

BLOCK = 1024
SUB = 128
KMAX = 24
CYCLE = 64
DMIN = 6
STEPS = 6
SENS = 128
REPS = 32
OWNERS = 32
COLUMNS = 8
BLOCKS = 256
NODES = 262144
CAP = 1
PIECES = 8


def draw_initial(key, part):
    keys = jax.random.split(key, 6)
    shape = (REPS, NODES)
    lows = (0.0, 4.0, 0.0, -0.5, -0.5, -0.5)
    highs = (0.4, 16.0, 8.0, 0.5, 0.5, 0.5)
    rows = []
    for row_index in range(6):
        unit = jax.random.uniform(keys[row_index], shape, jnp.float32)
        rows.append(lows[row_index] + (highs[row_index] - lows[row_index]) * unit)
    return jnp.stack(rows)


def draw_src_group(key, part):
    keys = jax.random.split(key, BLOCKS)

    def one_row(row_key):
        order = jax.random.permutation(row_key, CAP * OWNERS)
        return (order[:KMAX] % OWNERS).astype(jnp.int32)
    return jax.vmap(one_row)(keys)


def draw_counts(key, part):
    first_key, second_key = jax.random.split(key)
    base_counts = jax.random.randint(first_key, (BLOCKS,), KMAX - KMAX // 3, KMAX + 1)
    full_block = jax.random.randint(second_key, (), 0, BLOCKS)
    return base_counts.at[full_block].set(KMAX).astype(jnp.int32)


def place_ends(array, own_key, smallest, top_value):
    longest = array.shape.index(max(array.shape))
    spots = []
    for shift in (0, 1):
        where = [jax.random.randint(jax.random.fold_in(own_key, axis), (), 0, length) for axis, length in enumerate(array.shape)]
        where[longest] = (where[longest] + shift) % array.shape[longest]
        spots.append(tuple(where))
    return array.at[spots[0]].set(smallest).at[spots[1]].set(top_value)


def levels(own_key, extent, cuts, smallest, largest):
    def one(position, blocks):
        heights = jax.random.uniform(jax.random.fold_in(jax.random.fold_in(own_key, 6), position), (blocks,), jnp.float32, smallest / len(cuts), largest / len(cuts))
        return jnp.repeat(jnp.exp(heights), extent[position] // blocks).reshape((-1,) + (1,) * (len(extent) - position - 1))

    loudness = one(*cuts[0])
    for cut in cuts[1:]:
        loudness = loudness * one(*cut)
    return loudness


def gaussian(own_key, dims, width, limit, cuts=(), kind=jnp.bfloat16):
    drawn = width * jax.random.normal(own_key, dims, jnp.float32)
    if cuts:
        drawn = drawn * levels(own_key, dims, cuts, -0.22, 0.18)
    return jnp.clip(drawn, -limit, limit).astype(kind)


def setup_inputs(seed: int = 0) -> dict:
    splits = jax.random.split(jax.random.key(seed), 10)
    initial = draw_initial(jax.random.fold_in(splits[9], 71), 0)
    afferent_noise_level = jnp.clip(jnp.exp(math.log(0.32) - 0.98082925 * jax.random.uniform(splits[1], (REPS, NODES), jnp.float32) ** levels(splits[1], (REPS, NODES), ((1, 256),), -0.2, 0.2)), 0.12, 0.32)
    history = jnp.clip(1.0 * jax.random.uniform(splits[2], (CYCLE, REPS, NODES), jnp.float32) ** levels(splits[2], (CYCLE, REPS, NODES), ((2, 256),), -0.2, 0.2), 0.0, 1.0).astype(jnp.bfloat16)
    weights = gaussian(splits[3], (BLOCKS, KMAX, SUB, BLOCK), (KMAX * SUB) ** -0.5, 0.109375, ((0, 256),))
    lead_field = gaussian(splits[4], (SENS, NODES), (64 * NODES) ** -0.5, 0.0014648438, ((1, 256),))
    src_group = draw_src_group(jax.random.fold_in(splits[9], 71), 0)
    src_sub = place_ends(jax.random.randint(splits[6], (BLOCKS, KMAX), 0, PIECES), jax.random.fold_in(splits[6], 1), 0, PIECES - 1).astype(jnp.int32)
    delays = place_ends(jax.random.randint(splits[7], (BLOCKS, KMAX), DMIN, CYCLE), jax.random.fold_in(splits[7], 1), DMIN, CYCLE - 1).astype(jnp.int32)
    counts = draw_counts(jax.random.fold_in(splits[9], 71), 0)
    return dict(initial=initial, afferent_noise_level=afferent_noise_level, history=history, weights=weights, lead_field=lead_field, src_group=src_group, src_sub=src_sub, delays=delays, counts=counts)


exciting_amplitude = 3.25
suppressive_amplitude = 22.0
exciting_inverse_lag = 0.1
suppressive_inverse_lag = 0.05
link_factor = 135.0
maximal_spike_frequency = 0.005
thresh = 6.0
fire_slope = 0.56
global_scaling_factor = 0.5
dt_step = 0.5


def sigmoid_spike_density(somatic_charge_level):
    return 1.0 / (1.0 + jnp.exp(fire_slope * (thresh - somatic_charge_level)))


def derivative(population_variables, afferent_noise_level, network_afferent):
    principal_cell_level, interneuron_depolarization, suppressive_depolarization = population_variables[0], population_variables[1], population_variables[2]
    principal_cell_curvature = exciting_amplitude * exciting_inverse_lag * maximal_spike_frequency * sigmoid_spike_density(interneuron_depolarization - suppressive_depolarization) - 2.0 * exciting_inverse_lag * population_variables[3] - exciting_inverse_lag * exciting_inverse_lag * principal_cell_level
    interneuron_second_derivative = exciting_amplitude * exciting_inverse_lag * (afferent_noise_level + 0.8 * link_factor * maximal_spike_frequency * sigmoid_spike_density(link_factor * principal_cell_level) + global_scaling_factor * network_afferent) - 2.0 * exciting_inverse_lag * population_variables[4] - exciting_inverse_lag * exciting_inverse_lag * interneuron_depolarization
    suppressive_second_derivative = suppressive_amplitude * suppressive_inverse_lag * 0.25 * link_factor * maximal_spike_frequency * sigmoid_spike_density(0.25 * link_factor * principal_cell_level) - 2.0 * suppressive_inverse_lag * population_variables[5] - suppressive_inverse_lag * suppressive_inverse_lag * suppressive_depolarization
    return jnp.stack([population_variables[3], population_variables[4], population_variables[5], principal_cell_curvature, interneuron_second_derivative, suppressive_second_derivative])


def advance(population_variables, afferent_noise_level, coupled_now, coupled_next):
    first_rate = derivative(population_variables, afferent_noise_level, coupled_now)
    second_rate = derivative(population_variables + dt_step * first_rate, afferent_noise_level, coupled_next)
    return population_variables + (0.5 * dt_step) * (first_rate + second_rate)


def gather_input(cycle, in_time, weights, src_group, src_sub, delays, counts):
    zero_index = jnp.zeros((), jnp.int32)
    tile_lanes = jnp.arange(KMAX, dtype=jnp.int32)
    column = jnp.arange(BLOCKS, dtype=jnp.int32) % COLUMNS
    starts = ((src_group * COLUMNS + column[:, None]) * BLOCK + src_sub * SUB).astype(jnp.int32)
    slot_ids = jnp.mod(in_time - delays, CYCLE).astype(jnp.int32)

    def cut_piece(slot_id, start_id):
        return lax.dynamic_slice(cycle, (slot_id, zero_index, start_id), (1, REPS, SUB))[0]

    def one_block(element):
        start_row, slot_row, live_count, tile_block = element
        pieces = jax.vmap(cut_piece)(slot_row, start_row)
        live_mask = (tile_lanes < live_count).astype(jnp.bfloat16)
        pieces = pieces * live_mask[:, None, None]
        flattened = jnp.transpose(pieces, (1, 0, 2)).reshape(REPS, KMAX * SUB)
        return jnp.dot(flattened, tile_block.reshape(KMAX * SUB, BLOCK), preferred_element_type=jnp.float32)

    products = lax.map(one_block, (starts, slot_ids, counts, weights), batch_size=8)
    return jnp.transpose(products, (1, 0, 2)).reshape(REPS, BLOCKS * BLOCK)


def reference(initial, afferent_noise_level, history, weights, lead_field, src_group, src_sub, delays, counts):
    zero_index = jnp.zeros((), jnp.int32)

    def inputs(cycle, in_time):
        return gather_input(cycle, in_time, weights, src_group, src_sub, delays, counts)

    def record(sensors, population_variables, step_id):
        potential = (population_variables[1] - population_variables[2]).astype(jnp.bfloat16)
        local_sum = lax.dot_general(lead_field, potential, (((1,), (1,)), ((), ())), preferred_element_type=jnp.float32)
        return lax.dynamic_update_slice(sensors, local_sum[None], (step_id, zero_index, zero_index))

    network_afferent = inputs(history, jnp.zeros((), jnp.int32))
    sensors = jnp.zeros((STEPS, SENS, REPS), jnp.float32)

    def one_step(step_id, carried):
        population_variables, cycle, coupled_now, sensors = carried
        step_id = jnp.asarray(step_id).astype(jnp.int32)
        spike_density_result = sigmoid_spike_density(population_variables[1] - population_variables[2]).astype(jnp.bfloat16)
        cycle = lax.dynamic_update_slice(cycle, spike_density_result[None], (jnp.mod(step_id, CYCLE).astype(jnp.int32), zero_index, zero_index))
        coupled_next = inputs(cycle, step_id + 1)
        population_variables = advance(population_variables, afferent_noise_level, coupled_now, coupled_next)
        return population_variables, cycle, coupled_next, record(sensors, population_variables, step_id)

    population_variables, cycle, network_afferent, sensors = lax.fori_loop(0, STEPS, one_step, (initial, history, network_afferent, sensors))
    return population_variables, sensors
```

```python
import functools

import jax
import jax.numpy as jnp
from jax import lax
from jax.experimental import pallas as pl
from jax.experimental.pallas import tpu as pltpu
from jax.sharding import Mesh
from jax.sharding import PartitionSpec as P

STEPS = 6
GRP = ("grp_0", "grp_1")
NODE = ("node_0", "node_1")
GRP_NODE = ("grp_0", "grp_1", "node_0", "node_1")

DT = 0.5


def firing(v):
    return 1.0 / (1.0 + jnp.exp(0.56 * (6.0 - v)))


def pack_kernel(codes, column, history, out, sems, *, owners, columns, piece):
    def parcel(g):
        code = codes[g * columns + column[0]]
        return pltpu.make_async_copy(
            history.at[pl.ds(code // 8, STEPS), :, pl.ds((code % 8) * piece, piece)],
            out.at[g],
            sems.at[g],
        )

    for g in range(owners):
        parcel(g).start()
    for g in range(owners):
        parcel(g).wait()


def pack_last_kernel(
    codes, column, history, initial, out, rows, fire, sems, row_sem, *, owners, columns, piece, cycle
):
    load = pltpu.make_async_copy(initial.at[pl.ds(1, 2)], rows, row_sem)
    load.start()
    load.wait()
    fire[...] = firing(rows[0] - rows[1]).astype(fire.dtype)

    def old(g, code):
        slot = jnp.minimum(code // 8 + STEPS, cycle - 1)
        return pltpu.make_async_copy(
            history.at[slot, :, pl.ds((code % 8) * piece, piece)], out.at[g], sems.at[g]
        )

    def new(g, code):
        return pltpu.make_async_copy(
            fire.at[:, pl.ds((code % 8) * piece, piece)], out.at[g], sems.at[g]
        )

    for g in range(owners):
        code = codes[g * columns + column[0]]

        @pl.when(code // 8 + STEPS >= cycle)
        def _():
            new(g, code).start()

        @pl.when(code // 8 + STEPS < cycle)
        def _():
            old(g, code).start()

    for g in range(owners):
        old(g, codes[g * columns + column[0]]).wait()


def fill_left(own, parcel, left, tiles, piece):
    rows = left.shape[0]
    for k in range(tiles):
        group = own[k]
        got = parcel[jnp.maximum(group, 0)].reshape(rows, piece)
        left[:, k * piece : (k + 1) * piece] = jnp.where(group >= 0, got, jnp.zeros_like(got))


def second_derivatives(y, noise, coupled):
    d3 = 3.25 * 0.1 * 0.005 * firing(y[1] - y[2]) - 2.0 * 0.1 * y[3] - 0.1 * 0.1 * y[0]
    drive = noise + 0.8 * 135.0 * 0.005 * firing(135.0 * y[0])
    if coupled is not None:
        drive = drive + 0.5 * coupled
    d4 = 3.25 * 0.1 * drive - 2.0 * 0.1 * y[4] - 0.1 * 0.1 * y[1]
    d5 = (
        22.0 * 0.05 * 0.25 * 135.0 * 0.005 * firing(0.25 * 135.0 * y[0])
        - 2.0 * 0.05 * y[5]
        - 0.05 * 0.05 * y[2]
    )
    return d3, d4, d5


def evolve_kernel(
    own, parcel, weights, initial, noise, lead, state, sensors, left, coupled, potential, *, tiles, piece
):
    replicas, nodes = noise.shape
    fill_left(own, parcel, left, tiles, piece)
    coupled[...] = jnp.dot(
        left[...], weights[...].reshape(tiles * piece, nodes), preferred_element_type=jnp.float32
    )
    width = 128

    def strip(i, carry):
        lanes = pl.ds(pl.multiple_of(i * width, width), width)
        y = [initial[r, :, lanes] for r in range(6)]
        p = noise[:, lanes]
        for s in range(STEPS):
            now = coupled[s * replicas : (s + 1) * replicas, lanes]
            then = None
            if s + 1 < STEPS:
                then = coupled[(s + 1) * replicas : (s + 2) * replicas, lanes]
            first = (y[3], y[4], y[5], *second_derivatives(y, p, now))
            mid = [a + DT * b for a, b in zip(y, first)]
            second = (mid[3], mid[4], mid[5], *second_derivatives(mid, p, then))
            y = [a + 0.5 * DT * (b + c) for a, b, c in zip(y, first, second)]
            potential[s * replicas : (s + 1) * replicas, lanes] = (y[1] - y[2]).astype(
                potential.dtype
            )
        for r in range(6):
            state[r, :, lanes] = y[r]
        return carry

    lax.fori_loop(0, nodes // width, strip, 0)
    sensors[...] = lax.dot_general(
        potential[...], lead[...], (((1,), (1,)), ((), ())), preferred_element_type=jnp.float32
    )


def finish_kernel(own, parcel, weights, before, after, left, row, sem_in, sem_out, *, tiles, piece):
    load = pltpu.make_async_copy(before.at[4], row, sem_in)
    load.start()
    fill_left(own, parcel, left, tiles, piece)
    nodes = row.shape[1]
    coupled = jnp.dot(
        left[...], weights[...].reshape(tiles * piece, nodes), preferred_element_type=jnp.float32
    )
    load.wait()
    row[...] = row[...] + 0.5 * DT * (3.25 * 0.1 * 0.5) * coupled
    store = pltpu.make_async_copy(row, after.at[4], sem_out)
    store.start()
    store.wait()


def to_all(x, axis):
    copies = jnp.broadcast_to(x, (lax.axis_size(axis), *x.shape))
    return lax.all_to_all(copies, axis, split_axis=0, concat_axis=0, tiled=True)


def total_of(x):
    columns = lax.axis_size(NODE)
    parts = x.reshape(columns, -1, x.shape[-1])
    mine = jnp.sum(lax.all_to_all(parts, NODE, split_axis=0, concat_axis=0, tiled=True), axis=0)
    mine = jnp.sum(to_all(mine, GRP), axis=0)
    return to_all(mine, NODE).reshape(x.shape)


def body(
    initial, afferent_noise_level, history, weights, lead_field, src_group, src_sub, delays, counts
):
    owners = lax.axis_size(GRP)
    columns = lax.axis_size(NODE)
    my_group = lax.axis_index(GRP)
    my_column = lax.axis_index(NODE)
    myself = my_group * columns + my_column
    cycle, replicas, nodes = history.shape
    tiles, piece = weights.shape[1:3]
    sensors_count = lead_field.shape[0]
    lanes = jnp.arange(tiles, dtype=jnp.int32)

    group_t, sub_t, delay_t = src_group.T, src_sub.T, delays.T
    live = lanes[:, None] < counts[None, :]
    codes = jnp.sum(
        jnp.where((group_t == my_group) & live, (cycle - delay_t) * 8 + sub_t, 0), axis=0
    )
    column = my_column.astype(jnp.int32).reshape(1)
    own_group = lax.dynamic_index_in_dim(group_t, myself, 1, False)
    own_count = lax.dynamic_index_in_dim(counts, myself, 0, False)
    own = jnp.where(lanes < own_count, own_group, -1)

    smem = pl.BlockSpec(memory_space=pltpu.SMEM)
    vmem = pl.BlockSpec(memory_space=pltpu.VMEM)
    anywhere = pl.BlockSpec(memory_space=pl.ANY)
    bf16, f32 = jnp.bfloat16, jnp.float32
    sizes = dict(owners=owners, columns=columns, piece=piece)

    packed = pl.pallas_call(
        functools.partial(pack_kernel, **sizes),
        out_shape=jax.ShapeDtypeStruct((owners, STEPS, replicas, piece), bf16),
        in_specs=[smem, smem, anywhere],
        out_specs=anywhere,
        scratch_shapes=[pltpu.SemaphoreType.DMA((owners,))],
        name="pack",
    )(codes, column, history)
    packed_last = pl.pallas_call(
        functools.partial(pack_last_kernel, cycle=cycle, **sizes),
        out_shape=jax.ShapeDtypeStruct((owners, replicas, piece), bf16),
        in_specs=[smem, smem, anywhere, anywhere],
        out_specs=anywhere,
        scratch_shapes=[
            pltpu.VMEM((2, replicas, nodes), f32),
            pltpu.VMEM((replicas, nodes), bf16),
            pltpu.SemaphoreType.DMA((owners,)),
            pltpu.SemaphoreType.DMA,
        ],
        name="pack_last",
    )(codes, column, history, initial)
    parcel = lax.all_to_all(packed, GRP, split_axis=0, concat_axis=0, tiled=True)
    parcel_last = lax.all_to_all(packed_last, GRP, split_axis=0, concat_axis=0, tiled=True)

    tile_stack = weights.reshape(tiles, piece, nodes)
    shape = dict(tiles=tiles, piece=piece)
    state, local = pl.pallas_call(
        functools.partial(evolve_kernel, **shape),
        out_shape=(
            jax.ShapeDtypeStruct(initial.shape, f32),
            jax.ShapeDtypeStruct((STEPS * replicas, sensors_count), f32),
        ),
        in_specs=[smem, vmem, vmem, vmem, vmem, vmem],
        out_specs=(vmem, vmem),
        scratch_shapes=[
            pltpu.VMEM((STEPS * replicas, tiles * piece), bf16),
            pltpu.VMEM((STEPS * replicas, nodes), f32),
            pltpu.VMEM((STEPS * replicas, nodes), bf16),
        ],
        name="evolve",
    )(own, parcel, tile_stack, initial, afferent_noise_level, lead_field)

    total = total_of(local)
    sensors = jnp.transpose(total.reshape(STEPS, replicas, sensors_count), (0, 2, 1))

    final_state = pl.pallas_call(
        functools.partial(finish_kernel, **shape),
        out_shape=jax.ShapeDtypeStruct(initial.shape, f32),
        in_specs=[smem, vmem, vmem, anywhere],
        out_specs=anywhere,
        scratch_shapes=[
            pltpu.VMEM((replicas, tiles * piece), bf16),
            pltpu.VMEM((replicas, nodes), f32),
            pltpu.SemaphoreType.DMA,
            pltpu.SemaphoreType.DMA,
        ],
        input_output_aliases={3: 0},
        name="finish",
    )(own, parcel_last, tile_stack, state)
    return final_state, sensors


def solution(mesh):
    finer = Mesh(mesh.devices.reshape(4, 8, 4, 2), GRP_NODE)
    placed = (
        P(None, None, GRP_NODE),
        P(None, GRP_NODE),
        P(None, None, GRP_NODE),
        P(GRP_NODE, None, None, None),
        P(None, GRP_NODE),
        P(),
        P(),
        P(),
        P(),
    )
    return jax.shard_map(
        body, mesh=finer, in_specs=placed, out_specs=(P(None, None, GRP_NODE), P()), check_vma=False
    )
```

```python
import functools

import jax
import jax.numpy as jnp
from jax import lax
from jax.experimental import pallas as pl
from jax.experimental.pallas import tpu as pltpu
from jax.sharding import Mesh
from jax.sharding import PartitionSpec as P

STEPS = 6
GRP = ("grp_0", "grp_1")
NODE = ("node_0", "node_1")
GRP_NODE = ("grp_0", "grp_1", "node_0", "node_1")

DT = 0.5
MIB = 1 << 20


def firing(v):
    return 1.0 / (1.0 + jnp.exp(0.56 * (6.0 - v)))


def pack_kernel(
    codes, column, history, initial, out, last, rows, fire, sems, last_sems, row_sem, *, owners, columns, piece, cycle
):
    load = pltpu.make_async_copy(initial.at[pl.ds(1, 2)], rows, row_sem)
    load.start()

    def parcel(g, code):
        return pltpu.make_async_copy(
            history.at[pl.ds(code // 8, STEPS), :, pl.ds((code % 8) * piece, piece)],
            out.at[g],
            sems.at[g],
        )

    def old(g, code):
        slot = jnp.minimum(code // 8 + STEPS, cycle - 1)
        return pltpu.make_async_copy(
            history.at[slot, :, pl.ds((code % 8) * piece, piece)], last.at[g], last_sems.at[g]
        )

    def new(g, code):
        return pltpu.make_async_copy(
            fire.at[:, pl.ds((code % 8) * piece, piece)], last.at[g], last_sems.at[g]
        )

    for g in range(owners):
        parcel(g, codes[g * columns + column[0]]).start()
    load.wait()
    fire[...] = firing(rows[0] - rows[1]).astype(fire.dtype)
    for g in range(owners):
        code = codes[g * columns + column[0]]

        @pl.when(code // 8 + STEPS >= cycle)
        def _():
            new(g, code).start()

        @pl.when(code // 8 + STEPS < cycle)
        def _():
            old(g, code).start()

    for g in range(owners):
        code = codes[g * columns + column[0]]
        parcel(g, code).wait()
        old(g, code).wait()


def fill_left(own, parcel, left, tiles, piece):
    rows = left.shape[0]
    for k in range(tiles):
        group = own[k]
        got = parcel[jnp.maximum(group, 0)].reshape(rows, piece)
        left[:, k * piece : (k + 1) * piece] = jnp.where(group >= 0, got, jnp.zeros_like(got))


def second_derivatives(y, noise, coupled):
    d3 = 3.25 * 0.1 * 0.005 * firing(y[1] - y[2]) - 2.0 * 0.1 * y[3] - 0.1 * 0.1 * y[0]
    drive = noise + 0.8 * 135.0 * 0.005 * firing(135.0 * y[0])
    if coupled is not None:
        drive = drive + 0.5 * coupled
    d4 = 3.25 * 0.1 * drive - 2.0 * 0.1 * y[4] - 0.1 * 0.1 * y[1]
    d5 = (
        22.0 * 0.05 * 0.25 * 135.0 * 0.005 * firing(0.25 * 135.0 * y[0])
        - 2.0 * 0.05 * y[5]
        - 0.05 * 0.05 * y[2]
    )
    return d3, d4, d5


def evolve_kernel(
    own, parcel, weights, initial, noise, lead, state, sensors,
    stack, start, rate, gains, left, coupled, potential, sems, *, tiles, piece, pieces_at_once
):
    replicas, nodes = noise.shape
    chunks = tiles // pieces_at_once
    loads = [
        pltpu.make_async_copy(
            weights.at[pl.ds(i * pieces_at_once, pieces_at_once)],
            stack.at[pl.ds(i * pieces_at_once, pieces_at_once)],
            sems.at[i],
        )
        for i in range(chunks)
    ]
    others = [
        pltpu.make_async_copy(initial, start, sems.at[chunks]),
        pltpu.make_async_copy(noise, rate, sems.at[chunks + 1]),
        pltpu.make_async_copy(lead, gains, sems.at[chunks + 2]),
    ]
    for load in loads + others:
        load.start()
    fill_left(own, parcel, left, tiles, piece)
    depth = pieces_at_once * piece
    for i in range(chunks):
        loads[i].wait()
        part = jnp.dot(
            left[:, i * depth : (i + 1) * depth],
            stack[i * pieces_at_once : (i + 1) * pieces_at_once].reshape(depth, nodes),
            preferred_element_type=jnp.float32,
        )
        coupled[...] = part if i == 0 else coupled[...] + part
    for other in others:
        other.wait()
    width = 128

    def strip(i, carry):
        lanes = pl.ds(pl.multiple_of(i * width, width), width)
        y = [start[r, :, lanes] for r in range(6)]
        p = rate[:, lanes]
        for s in range(STEPS):
            now = coupled[s * replicas : (s + 1) * replicas, lanes]
            then = None
            if s + 1 < STEPS:
                then = coupled[(s + 1) * replicas : (s + 2) * replicas, lanes]
            first = (y[3], y[4], y[5], *second_derivatives(y, p, now))
            mid = [a + DT * b for a, b in zip(y, first)]
            second = (mid[3], mid[4], mid[5], *second_derivatives(mid, p, then))
            y = [a + 0.5 * DT * (b + c) for a, b, c in zip(y, first, second)]
            potential[s * replicas : (s + 1) * replicas, lanes] = (y[1] - y[2]).astype(
                potential.dtype
            )
        for r in range(6):
            state[r, :, lanes] = y[r]
        return carry

    lax.fori_loop(0, nodes // width, strip, 0)
    sensors[...] = lax.dot_general(
        potential[...], gains[...], (((1,), (1,)), ((), ())), preferred_element_type=jnp.float32
    )


def finish_kernel(own, parcel, weights, before, after, stack, left, sem, *, tiles, piece):
    load = pltpu.make_async_copy(weights, stack, sem)
    load.start()
    fill_left(own, parcel, left, tiles, piece)
    for r in (0, 1, 2, 3, 5):
        after[r] = before[r]
    load.wait()
    coupled = jnp.dot(
        left[...],
        stack[...].reshape(tiles * piece, before.shape[2]),
        preferred_element_type=jnp.float32,
    )
    after[4] = before[4] + 0.5 * DT * (3.25 * 0.1 * 0.5) * coupled


def to_all(x, axis):
    copies = jnp.broadcast_to(x, (lax.axis_size(axis), *x.shape))
    return lax.all_to_all(copies, axis, split_axis=0, concat_axis=0, tiled=True)


def total_of(x):
    columns = lax.axis_size(NODE)
    parts = x.reshape(columns, -1, x.shape[-1])
    mine = jnp.sum(lax.all_to_all(parts, NODE, split_axis=0, concat_axis=0, tiled=True), axis=0)
    mine = jnp.sum(to_all(mine, GRP), axis=0)
    return to_all(mine, NODE).reshape(x.shape)


def body(
    initial, afferent_noise_level, history, weights, lead_field, src_group, src_sub, delays, counts
):
    owners = lax.axis_size(GRP)
    columns = lax.axis_size(NODE)
    my_group = lax.axis_index(GRP)
    my_column = lax.axis_index(NODE)
    myself = my_group * columns + my_column
    cycle, replicas, nodes = history.shape
    tiles, piece = weights.shape[1:3]
    sensors_count = lead_field.shape[0]
    lanes = jnp.arange(tiles, dtype=jnp.int32)

    group_t, sub_t, delay_t = src_group.T, src_sub.T, delays.T
    live = lanes[:, None] < counts[None, :]
    codes = jnp.sum(
        jnp.where((group_t == my_group) & live, (cycle - delay_t) * 8 + sub_t, 0), axis=0
    )
    column = my_column.astype(jnp.int32).reshape(1)
    own_group = lax.dynamic_index_in_dim(group_t, myself, 1, False)
    own_count = lax.dynamic_index_in_dim(counts, myself, 0, False)
    own = jnp.where(lanes < own_count, own_group, -1)

    smem = pl.BlockSpec(memory_space=pltpu.SMEM)
    vmem = pl.BlockSpec(memory_space=pltpu.VMEM)
    far = pl.BlockSpec(memory_space=pltpu.HBM)
    bf16, f32 = jnp.bfloat16, jnp.float32

    def near(x):
        return pltpu.with_memory_space_constraint(x, pltpu.VMEM)

    def outside(x):
        return pltpu.with_memory_space_constraint(x, pltpu.HBM)


    packed, packed_last = pl.pallas_call(
        functools.partial(
            pack_kernel, owners=owners, columns=columns, piece=piece, cycle=cycle
        ),
        out_shape=(
            pltpu.VMEM((owners, STEPS, replicas, piece), bf16),
            pltpu.VMEM((owners, replicas, piece), bf16),
        ),
        in_specs=[smem, smem, far, far],
        out_specs=(vmem, vmem),
        scratch_shapes=[
            pltpu.VMEM((2, replicas, nodes), f32),
            pltpu.VMEM((replicas, nodes), bf16),
            pltpu.SemaphoreType.DMA((owners,)),
            pltpu.SemaphoreType.DMA((owners,)),
            pltpu.SemaphoreType.DMA,
        ],
        compiler_params=pltpu.CompilerParams(vmem_limit_bytes=4 * MIB),
        name="pack",
    )(codes, column, outside(history), outside(initial))
    parcel = lax.all_to_all(packed, GRP, split_axis=0, concat_axis=0, tiled=True)
    parcel_last = lax.all_to_all(packed_last, GRP, split_axis=0, concat_axis=0, tiled=True)

    tile_stack = outside(weights.reshape(tiles, piece, nodes))
    shape = dict(tiles=tiles, piece=piece)
    state, local = pl.pallas_call(
        functools.partial(evolve_kernel, pieces_at_once=6, **shape),
        out_shape=(
            pltpu.VMEM(initial.shape, f32),
            pltpu.VMEM((STEPS * replicas, sensors_count), f32),
        ),
        in_specs=[smem, vmem, far, far, far, far],
        out_specs=(vmem, vmem),
        scratch_shapes=[
            pltpu.VMEM(tile_stack.shape, bf16),
            pltpu.VMEM(initial.shape, f32),
            pltpu.VMEM(afferent_noise_level.shape, f32),
            pltpu.VMEM(lead_field.shape, bf16),
            pltpu.VMEM((STEPS * replicas, tiles * piece), bf16),
            pltpu.VMEM((STEPS * replicas, nodes), f32),
            pltpu.VMEM((STEPS * replicas, nodes), bf16),
            pltpu.SemaphoreType.DMA((tiles // 6 + 3,)),
        ],
        compiler_params=pltpu.CompilerParams(vmem_limit_bytes=24 * MIB),
        name="evolve",
    )(own, near(parcel), tile_stack, outside(initial), outside(afferent_noise_level), outside(lead_field))

    total = total_of(local)
    sensors = jnp.transpose(total.reshape(STEPS, replicas, sensors_count), (0, 2, 1))

    final_state = pl.pallas_call(
        functools.partial(finish_kernel, **shape),
        out_shape=jax.ShapeDtypeStruct(initial.shape, f32),
        in_specs=[smem, vmem, far, vmem],
        out_specs=vmem,
        scratch_shapes=[
            pltpu.VMEM(tile_stack.shape, bf16),
            pltpu.VMEM((replicas, tiles * piece), bf16),
            pltpu.SemaphoreType.DMA,
        ],
        compiler_params=pltpu.CompilerParams(vmem_limit_bytes=24 * MIB),
        name="finish",
    )(own, near(parcel_last), tile_stack, near(state))
    return final_state, sensors


def solution(mesh):
    finer = Mesh(mesh.devices.reshape(4, 8, 4, 2), GRP_NODE)
    placed = (
        P(None, None, GRP_NODE),
        P(None, GRP_NODE),
        P(None, None, GRP_NODE),
        P(GRP_NODE, None, None, None),
        P(None, GRP_NODE),
        P(),
        P(),
        P(),
        P(),
    )
    return jax.shard_map(
        body, mesh=finer, in_specs=placed, out_specs=(P(None, None, GRP_NODE), P()), check_vma=False
    )
```

```python
import functools

import jax
import jax.numpy as jnp
from jax import lax
from jax.experimental import pallas as pl
from jax.experimental.pallas import tpu as pltpu
from jax.sharding import Mesh
from jax.sharding import PartitionSpec as P

STEPS = 6
TIMES = STEPS + 1
GRP = ("grp_0", "grp_1")
NODE = ("node_0", "node_1")
GRP_NODE = ("grp_0", "grp_1", "node_0", "node_1")

DT = 0.5
MIB = 1 << 20


def firing(v):
    return 1.0 / (1.0 + jnp.exp(0.56 * (6.0 - v)))


def pack_kernel(
    codes, column, history, initial, out, parts, rows, fire, gets, puts, row_sem, *, owners, columns, piece, cycle
):
    replicas = fire.shape[0]
    load = pltpu.make_async_copy(initial.at[pl.ds(1, 2)], rows, row_sem)
    load.start()

    def code_of(g):
        return codes[g * columns + column[0]]

    def get(g):
        start = jnp.minimum((code_of(g) >> 3), cycle - TIMES)
        sub = (code_of(g) & 7) * piece
        return pltpu.make_async_copy(
            history.at[pl.ds(start, TIMES), :, pl.ds(sub, piece)], parts.at[g], gets.at[g]
        )

    def put(g):
        return pltpu.make_async_copy(parts.at[g], out.at[g], puts.at[g])

    def reaches(g):
        return (code_of(g) >> 3) + TIMES > cycle

    for g in range(owners):
        get(g).start()
    load.wait()
    fire[...] = firing(rows[0] - rows[1]).astype(fire.dtype)
    for g in range(owners):
        get(g).wait()

        @pl.when(reaches(g))
        def _():
            sub = pl.multiple_of((code_of(g) & 7) * piece, piece)
            for t in range(TIMES - 1):
                parts[g, t] = parts[g, t + 1]
            parts[g, TIMES - 1] = fire[:, pl.ds(sub, piece)]

        put(g).start()
    for g in range(owners):
        put(g).wait()


def fill_left(own, parcel, left, tiles, piece):
    rows = left.shape[0]
    for k in range(tiles):
        group = own[k]
        got = parcel[jnp.maximum(group, 0)].reshape(rows, piece)
        left[:, k * piece : (k + 1) * piece] = jnp.where(group >= 0, got, jnp.zeros_like(got))


Q = 0.5 * DT * DT
G0 = Q * 3.25 * 0.1 * 0.005 * 0.5
G1 = Q * 3.25 * 0.1 * 0.8 * 135.0 * 0.005 * 0.5
G2 = Q * 22.0 * 0.05 * 0.25 * 135.0 * 0.005 * 0.5
DRIVE = Q * 3.25 * 0.1


def increments(y, z, drive):
    steep = (0.28 * 135.0) * y[0]
    t0 = jnp.tanh(0.28 * (y[1] - y[2]) - 1.68)
    t1 = jnp.tanh(steep - 1.68)
    t2 = jnp.tanh(0.25 * steep - 1.68)
    return (
        G0 * t0 + G0 - (Q * 0.2 / DT) * z[0] - (Q * 0.01) * y[0],
        G1 * t1 + drive - (Q * 0.2 / DT) * z[1] - (Q * 0.01) * y[1],
        G2 * t2 + G2 - (Q * 0.1 / DT) * z[2] - (Q * 0.0025) * y[2],
    )


def evolve_kernel(
    own, parcel, weights, initial, noise, lead, state, sensors,
    stack, start, rate, gains, left, coupled, potential, sems, *, tiles, piece, width, ahead
):
    replicas, nodes = noise.shape
    chunks = nodes // width
    loads = [
        pltpu.make_async_copy(weights.at[:, :, pl.ds(i * width, width)], stack.at[i], sems.at[i])
        for i in range(chunks)
    ]
    others = [
        pltpu.make_async_copy(initial, start, sems.at[chunks]),
        pltpu.make_async_copy(noise, rate, sems.at[chunks + 1]),
        pltpu.make_async_copy(lead, gains, sems.at[chunks + 2]),
    ]
    loads[0].start()
    for other in others:
        other.start()
    for load in loads[1:ahead]:
        load.start()
    fill_left(own, parcel, left, tiles, piece)
    lane = width

    def strip(i, carry):
        lanes = pl.ds(pl.multiple_of(i * lane, lane), lane)
        y = [start[r, :, lanes] for r in range(3)]
        z = [DT * start[r, :, lanes] for r in range(3, 6)]
        noisy = DRIVE * rate[:, lanes] + G1
        drives = [
            noisy + (0.5 * DRIVE) * coupled[t * replicas : (t + 1) * replicas, lanes]
            for t in range(2)
        ]
        for s in range(STEPS):
            w = increments(y, z, drives[s])
            y = [a + b for a, b in zip(y, z)]
            part = [a + b for a, b in zip(z, w)]
            second = increments(y, [a + b for a, b in zip(part, w)], drives[s + 1])
            y = [a + b for a, b in zip(y, w)]
            z = [a + b for a, b in zip(part, second)]
            potential[s * replicas : (s + 1) * replicas, lanes] = (y[1] - y[2]).astype(
                potential.dtype
            )
            if s + 2 < TIMES:
                drives.append(
                    noisy
                    + (0.5 * DRIVE) * coupled[(s + 2) * replicas : (s + 3) * replicas, lanes]
                )
        for r in range(3):
            state[r, :, lanes] = y[r]
            state[r + 3, :, lanes] = (1.0 / DT) * z[r]
        return carry

    for i in range(chunks):
        loads[i].wait()
        if i + ahead < chunks:
            loads[i + ahead].start()
        coupled[:, i * width : (i + 1) * width] = jnp.dot(
            left[...],
            stack[i].reshape(tiles * piece, width),
            preferred_element_type=jnp.float32,
        )
        if i == 0:
            for other in others:
                other.wait()
        lax.fori_loop(i * width // lane, (i + 1) * width // lane, strip, 0)
    sensors[...] = lax.dot_general(
        potential[...], gains[...], (((1,), (1,)), ((), ())), preferred_element_type=jnp.float32
    )


def to_all(x, axis):
    copies = jnp.broadcast_to(x, (lax.axis_size(axis), *x.shape))
    return lax.all_to_all(copies, axis, split_axis=0, concat_axis=0, tiled=True)


def total_of(x):
    columns = lax.axis_size(NODE)
    parts = x.reshape(columns, -1, x.shape[-1])
    mine = jnp.sum(lax.all_to_all(parts, NODE, split_axis=0, concat_axis=0, tiled=True), axis=0)
    mine = jnp.sum(to_all(mine, GRP), axis=0)
    return to_all(mine, NODE).reshape(x.shape)


def body(
    initial, afferent_noise_level, history, weights, lead_field, src_group, src_sub, delays, counts
):
    owners = lax.axis_size(GRP)
    columns = lax.axis_size(NODE)
    my_group = lax.axis_index(GRP)
    my_column = lax.axis_index(NODE)
    myself = my_group * columns + my_column
    cycle, replicas, nodes = history.shape
    tiles, piece = weights.shape[1:3]
    sensors_count = lead_field.shape[0]
    lanes = jnp.arange(tiles, dtype=jnp.int32)

    group_t, sub_t, delay_t = src_group.T, src_sub.T, delays.T
    live = lanes[:, None] < counts[None, :]
    codes = jnp.sum(
        jnp.where((group_t == my_group) & live, (cycle - delay_t) * 8 + sub_t, 0), axis=0
    )
    column = my_column.astype(jnp.int32).reshape(1)
    mine = (jnp.arange(counts.shape[0], dtype=jnp.int32) == myself)[None, :] & live
    own = jnp.sum(jnp.where(mine, group_t + 1, 0), axis=1) - 1

    smem = pl.BlockSpec(memory_space=pltpu.SMEM)
    vmem = pl.BlockSpec(memory_space=pltpu.VMEM)
    far = pl.BlockSpec(memory_space=pltpu.HBM)
    bf16, f32 = jnp.bfloat16, jnp.float32

    def near(x):
        return pltpu.with_memory_space_constraint(x, pltpu.VMEM)

    def outside(x):
        return pltpu.with_memory_space_constraint(x, pltpu.HBM)


    packed = pl.pallas_call(
        functools.partial(
            pack_kernel, owners=owners, columns=columns, piece=piece, cycle=cycle
        ),
        out_shape=pltpu.HBM((owners, TIMES, replicas, piece), bf16),
        in_specs=[smem, smem, far, far],
        out_specs=far,
        scratch_shapes=[
            pltpu.VMEM((owners, TIMES, replicas, piece), bf16),
            pltpu.VMEM((2, replicas, nodes), f32),
            pltpu.VMEM((replicas, nodes), bf16),
            pltpu.SemaphoreType.DMA((owners,)),
            pltpu.SemaphoreType.DMA((owners,)),
            pltpu.SemaphoreType.DMA,
        ],
        compiler_params=pltpu.CompilerParams(vmem_limit_bytes=8 * MIB),
        name="pack",
    )(codes, column, outside(history), outside(initial))
    parcel = lax.all_to_all(packed, GRP, split_axis=0, concat_axis=0, tiled=True)

    tile_stack = outside(weights.reshape(tiles, piece, nodes))
    width = 512
    state, local = pl.pallas_call(
        functools.partial(evolve_kernel, tiles=tiles, piece=piece, width=width, ahead=2),
        out_shape=(
            pltpu.VMEM(initial.shape, f32),
            pltpu.VMEM((STEPS * replicas, sensors_count), f32),
        ),
        in_specs=[smem, vmem, far, far, far, far],
        out_specs=(vmem, vmem),
        scratch_shapes=[
            pltpu.VMEM((nodes // width, tiles, piece, width), bf16),
            pltpu.VMEM(initial.shape, f32),
            pltpu.VMEM(afferent_noise_level.shape, f32),
            pltpu.VMEM(lead_field.shape, bf16),
            pltpu.VMEM((TIMES * replicas, tiles * piece), bf16),
            pltpu.VMEM((TIMES * replicas, nodes), f32),
            pltpu.VMEM((STEPS * replicas, nodes), bf16),
            pltpu.SemaphoreType.DMA((nodes // width + 3,)),
        ],
        compiler_params=pltpu.CompilerParams(vmem_limit_bytes=24 * MIB),
        name="evolve",
    )(own, near(parcel), tile_stack, outside(initial), outside(afferent_noise_level), outside(lead_field))

    total = total_of(local)
    sensors = jnp.transpose(total.reshape(STEPS, replicas, sensors_count), (0, 2, 1))
    return state, sensors


def solution(mesh):
    finer = Mesh(mesh.devices.reshape(4, 8, 4, 2), GRP_NODE)
    placed = (
        P(None, None, GRP_NODE),
        P(None, GRP_NODE),
        P(None, None, GRP_NODE),
        P(GRP_NODE, None, None, None),
        P(None, GRP_NODE),
        P(),
        P(),
        P(),
        P(),
    )
    return jax.shard_map(
        body, mesh=finer, in_specs=placed, out_specs=(P(None, None, GRP_NODE), P()), check_vma=False
    )
```

```python
import functools

import jax
import jax.numpy as jnp
from jax import lax
from jax.experimental import pallas as pl
from jax.experimental.pallas import tpu as pltpu
from jax.sharding import Mesh
from jax.sharding import PartitionSpec as P

STEPS = 6
TIMES = STEPS + 1
GRP = ("grp_0", "grp_1", "grp_2")
NODE = ("node_0", "node_1")
GRP_NODE = GRP + NODE
SPREAD = ("grp_1", "node_0", "node_1")
REST = ("grp_0", "grp_2")

DT = 0.5
MIB = 1 << 20


def firing(v):
    return 1.0 / (1.0 + jnp.exp(0.56 * (6.0 - v)))


def pack_kernel(
    codes, column, history, initial, out, parts, rows, fire, gets, puts, row_sem, *, owners, columns, piece, cycle
):
    replicas = fire.shape[0]
    load = pltpu.make_async_copy(initial.at[pl.ds(1, 2)], rows, row_sem)
    load.start()

    def code_of(g):
        return codes[g * columns + column[0]]

    def get(g):
        start = jnp.minimum((code_of(g) >> 3), cycle - TIMES)
        sub = (code_of(g) & 7) * piece
        return pltpu.make_async_copy(
            history.at[pl.ds(start, TIMES), :, pl.ds(sub, piece)], parts.at[g], gets.at[g]
        )

    def put(g):
        return pltpu.make_async_copy(parts.at[g], out.at[g], puts.at[g])

    def reaches(g):
        return (code_of(g) >> 3) + TIMES > cycle

    for g in range(owners):
        get(g).start()
    load.wait()
    fire[...] = firing(rows[0] - rows[1]).astype(fire.dtype)
    for g in range(owners):
        get(g).wait()

        @pl.when(reaches(g))
        def _():
            sub = pl.multiple_of((code_of(g) & 7) * piece, piece)
            for t in range(TIMES - 1):
                parts[g, t] = parts[g, t + 1]
            parts[g, TIMES - 1] = fire[:, pl.ds(sub, piece)]

        put(g).start()
    for g in range(owners):
        put(g).wait()


def fill_left(own, parcel, left, tiles, piece):
    rows = left.shape[0]
    for k in range(tiles):
        group = own[k]
        got = parcel[jnp.maximum(group, 0)].reshape(rows, piece)
        left[:, k * piece : (k + 1) * piece] = jnp.where(group >= 0, got, jnp.zeros_like(got))


Q = 0.5 * DT * DT
G0 = Q * 3.25 * 0.1 * 0.005 * 0.5
G1 = Q * 3.25 * 0.1 * 0.8 * 135.0 * 0.005 * 0.5
G2 = Q * 22.0 * 0.05 * 0.25 * 135.0 * 0.005 * 0.5
DRIVE = Q * 3.25 * 0.1


def increments(y, z, drive):
    steep = (0.28 * 135.0) * y[0]
    t0 = jnp.tanh(0.28 * (y[1] - y[2]) - 1.68)
    t1 = jnp.tanh(steep - 1.68)
    t2 = jnp.tanh(0.25 * steep - 1.68)
    return (
        G0 * t0 + G0 - (Q * 0.2 / DT) * z[0] - (Q * 0.01) * y[0],
        G1 * t1 + drive - (Q * 0.2 / DT) * z[1] - (Q * 0.01) * y[1],
        G2 * t2 + G2 - (Q * 0.1 / DT) * z[2] - (Q * 0.0025) * y[2],
    )


def hold_kernel(after, weights, held, sem):
    load = pltpu.make_async_copy(
        weights.at[pl.ds(0, held.shape[0]), :, pl.ds(0, held.shape[2])], held, sem
    )
    load.start()
    load.wait()


def evolve_kernel(
    own, parcel, held, weights, initial, noise, lead, state, sensors,
    stack, start, rate, gains, left, coupled, potential, sems, out_sems, *, tiles, piece, width
):
    replicas, nodes = noise.shape
    chunks = nodes // width
    early = held.shape[0]
    loads = [
        pltpu.make_async_copy(
            weights.at[pl.ds(first, tiles - first), :, pl.ds(i * width, width)],
            stack.at[i, pl.ds(first, tiles - first)],
            sems.at[i],
        )
        for i in range(chunks)
        for first in [0 if i else early]
    ]
    others = [
        pltpu.make_async_copy(initial, start, sems.at[chunks]),
        pltpu.make_async_copy(noise, rate, sems.at[chunks + 1]),
        pltpu.make_async_copy(lead, gains, sems.at[chunks + 2]),
    ]
    for load in (loads[0], *others, *loads[1:]):
        load.start()
    fill_left(own, parcel, left, tiles, piece)

    def strip(lanes):
        y = [start[r, :, lanes] for r in range(3)]
        z = [DT * start[r, :, lanes] for r in range(3, 6)]
        noisy = DRIVE * rate[:, lanes] + G1
        drives = [
            noisy + (0.5 * DRIVE) * coupled[t * replicas : (t + 1) * replicas, lanes]
            for t in range(2)
        ]
        for s in range(STEPS):
            w = increments(y, z, drives[s])
            y = [a + b for a, b in zip(y, z)]
            part = [a + b for a, b in zip(z, w)]
            second = increments(y, [a + b for a, b in zip(part, w)], drives[s + 1])
            y = [a + b for a, b in zip(y, w)]
            z = [a + b for a, b in zip(part, second)]
            potential[s * replicas : (s + 1) * replicas, lanes] = (y[1] - y[2]).astype(
                potential.dtype
            )
            if s + 2 < TIMES:
                drives.append(
                    noisy
                    + (0.5 * DRIVE) * coupled[(s + 2) * replicas : (s + 3) * replicas, lanes]
                )
        for r in range(3):
            start[r, :, lanes] = y[r]
            start[r + 3, :, lanes] = (1.0 / DT) * z[r]

    stores = []
    def product(first, some):
        depth = some.shape[0] * piece
        return jnp.dot(
            left[:, first * piece : first * piece + depth],
            some.reshape(depth, width),
            preferred_element_type=jnp.float32,
        )

    for i in range(chunks):
        lanes = slice(i * width, (i + 1) * width)
        if i:
            loads[i].wait()
            coupled[:, lanes] = product(0, stack[i])
        else:
            coupled[:, lanes] = product(0, held[...])
            loads[i].wait()
            coupled[:, lanes] = coupled[:, lanes] + product(early, stack[i, early:])
        if i == 0:
            for other in others:
                other.wait()
        strip(lanes)
        stores.append(
            pltpu.make_async_copy(
                start.at[:, :, lanes], state.at[:, :, lanes], out_sems.at[i]
            )
        )
        stores[-1].start()
    local = lax.dot_general(
        potential[...], gains[...], (((1,), (1,)), ((), ())), preferred_element_type=jnp.float32
    )
    sensors[...] = local.reshape(sensors.shape)
    for store in stores:
        store.wait()


def to_all(x, axis):
    copies = jnp.broadcast_to(x, (lax.axis_size(axis), *x.shape))
    return lax.all_to_all(copies, axis, split_axis=0, concat_axis=0, tiled=True)


def total_of(parts):
    mine = jnp.sum(lax.all_to_all(parts, SPREAD, split_axis=0, concat_axis=0, tiled=True), axis=0)
    mine = jnp.sum(to_all(mine, REST), axis=0)
    return to_all(mine, SPREAD)


def body(
    initial, afferent_noise_level, history, weights, lead_field, src_group, src_sub, delays, counts
):
    owners = lax.axis_size(GRP)
    columns = lax.axis_size(NODE)
    my_group = lax.axis_index(GRP)
    my_column = lax.axis_index(NODE)
    myself = my_group * columns + my_column
    cycle, replicas, nodes = history.shape
    tiles, piece = weights.shape[1:3]
    sensors_count = lead_field.shape[0]
    lanes = jnp.arange(tiles, dtype=jnp.int32)

    group_t, sub_t, delay_t = src_group.T, src_sub.T, delays.T
    live = lanes[:, None] < counts[None, :]
    codes = jnp.sum(
        jnp.where((group_t == my_group) & live, (cycle - delay_t) * 8 + sub_t, 0), axis=0
    )
    column = my_column.astype(jnp.int32).reshape(1)
    mine = (jnp.arange(counts.shape[0], dtype=jnp.int32) == myself)[None, :] & live
    own = jnp.sum(jnp.where(mine, group_t + 1, 0), axis=1) - 1

    smem = pl.BlockSpec(memory_space=pltpu.SMEM)
    vmem = pl.BlockSpec(memory_space=pltpu.VMEM)
    far = pl.BlockSpec(memory_space=pltpu.HBM)
    bf16, f32 = jnp.bfloat16, jnp.float32

    def near(x):
        return pltpu.with_memory_space_constraint(x, pltpu.VMEM)

    def outside(x):
        return pltpu.with_memory_space_constraint(x, pltpu.HBM)


    packed = pl.pallas_call(
        functools.partial(
            pack_kernel, owners=owners, columns=columns, piece=piece, cycle=cycle
        ),
        out_shape=pltpu.HBM((owners, TIMES, replicas, piece), bf16),
        in_specs=[smem, smem, far, far],
        out_specs=far,
        scratch_shapes=[
            pltpu.VMEM((owners, TIMES, replicas, piece), bf16),
            pltpu.VMEM((2, replicas, nodes), f32),
            pltpu.VMEM((replicas, nodes), bf16),
            pltpu.SemaphoreType.DMA((owners,)),
            pltpu.SemaphoreType.DMA((owners,)),
            pltpu.SemaphoreType.DMA,
        ],
        compiler_params=pltpu.CompilerParams(vmem_limit_bytes=8 * MIB),
        name="pack",
    )(codes, column, outside(history), outside(initial))
    parcel = lax.all_to_all(packed, GRP, split_axis=0, concat_axis=0, tiled=True)

    tile_stack = outside(weights.reshape(tiles, piece, nodes))
    width, early = nodes // 2, tiles // 2
    spread = lax.axis_size(SPREAD)
    chunks = nodes // width
    held = pl.pallas_call(
        hold_kernel,
        out_shape=pltpu.VMEM((early, piece, width), bf16),
        in_specs=[far, far],
        out_specs=vmem,
        scratch_shapes=[pltpu.SemaphoreType.DMA],
        compiler_params=pltpu.CompilerParams(vmem_limit_bytes=4 * MIB),
        name="hold",
    )(outside(packed), tile_stack)
    state, local = pl.pallas_call(
        functools.partial(evolve_kernel, tiles=tiles, piece=piece, width=width),
        out_shape=(
            pltpu.HBM(initial.shape, f32),
            pltpu.VMEM((spread, STEPS * replicas // spread, sensors_count), f32),
        ),
        in_specs=[smem, vmem, vmem, far, far, far, far],
        out_specs=(far, vmem),
        scratch_shapes=[
            pltpu.VMEM((chunks, tiles, piece, width), bf16),
            pltpu.VMEM(initial.shape, f32),
            pltpu.VMEM(afferent_noise_level.shape, f32),
            pltpu.VMEM(lead_field.shape, bf16),
            pltpu.VMEM((TIMES * replicas, tiles * piece), bf16),
            pltpu.VMEM((TIMES * replicas, nodes), f32),
            pltpu.VMEM((STEPS * replicas, nodes), bf16),
            pltpu.SemaphoreType.DMA((chunks + 3,)),
            pltpu.SemaphoreType.DMA((chunks,)),
        ],
        compiler_params=pltpu.CompilerParams(vmem_limit_bytes=32 * MIB),
        name="evolve",
    )(
        own,
        near(parcel),
        near(held),
        tile_stack,
        outside(initial),
        outside(afferent_noise_level),
        outside(lead_field),
    )

    total = total_of(local)
    sensors = jnp.transpose(total.reshape(STEPS, replicas, sensors_count), (0, 2, 1))
    return state, sensors


def solution(mesh):
    finer = Mesh(mesh.devices.reshape(2, 2, 8, 4, 2), GRP_NODE)
    placed = (
        P(None, None, GRP_NODE),
        P(None, GRP_NODE),
        P(None, None, GRP_NODE),
        P(GRP_NODE, None, None, None),
        P(None, GRP_NODE),
        P(),
        P(),
        P(),
        P(),
    )
    return jax.shard_map(
        body, mesh=finer, in_specs=placed, out_specs=(P(None, None, GRP_NODE), P()), check_vma=False
    )
```

```python
import functools

import jax
import jax.numpy as jnp
from jax import lax
from jax.experimental import pallas as pl
from jax.experimental.pallas import tpu as pltpu
from jax.sharding import Mesh
from jax.sharding import PartitionSpec as P

STEPS = 6
TIMES = STEPS + 1
GRP = ("grp_0", "grp_1", "grp_2")
NODE = ("node_0", "node_1")
GRP_NODE = GRP + NODE
SPREAD = ("grp_1", "node_0", "node_1")
REST = ("grp_0", "grp_2")

DT = 0.5
MIB = 1 << 20


def firing(v):
    return 1.0 / (1.0 + jnp.exp(0.56 * (6.0 - v)))


def pack_kernel(
    group, column, groups, subs, delays, counts, history, initial, out,
    whole, parts, rows, tables, limits, codes, chosen, gets, puts, row_sem, table_sems, code_sem, *, columns, piece
):
    owners = out.shape[0]
    tiles, blocks = tables.shape[1:]
    cycle = history.shape[0]
    some = cycle // gets.shape[0]
    loads = [
        pltpu.make_async_copy(
            history.at[pl.ds(i * some, some)], whole.at[pl.ds(i * some, some)], gets.at[i]
        )
        for i in range(gets.shape[0])
    ]
    load_rows = pltpu.make_async_copy(initial.at[pl.ds(1, 2)], rows, row_sem)
    lookups = [
        pltpu.make_async_copy(table, tables.at[i], table_sems.at[i])
        for i, table in enumerate((groups, subs, delays))
    ] + [pltpu.make_async_copy(counts, limits, table_sems.at[3])]
    for load in (*lookups, load_rows, *loads):
        load.start()
    for load in lookups:
        load.wait()
    lanes = lax.broadcasted_iota(jnp.int32, (tiles, blocks), 0)
    mine = (tables[0] == group[0]) & (lanes < limits[...])
    code = jnp.sum(jnp.where(mine, (cycle - tables[2]) * 8 + tables[1], 0), axis=0, keepdims=True)
    codes[...] = code
    move = pltpu.make_async_copy(codes, chosen, code_sem)
    move.start()
    load_rows.wait()
    whole[cycle] = firing(rows[0] - rows[1]).astype(whole.dtype)
    move.wait()
    for load in loads:
        load.wait()

    def put(g):
        return pltpu.make_async_copy(parts.at[g], out.at[g], puts.at[g])

    for g in range(owners):
        code = chosen[0, g * columns + column[0]]
        sub = pl.multiple_of((code & 7) * piece, piece)
        parts[g] = whole[pl.ds(code >> 3, TIMES), :, pl.ds(sub, piece)]
        put(g).start()
    for g in range(owners):
        put(g).wait()


def fill_left(own, parcel, left, tiles, piece):
    rows = left.shape[0]
    for k in range(tiles):
        group = own[k]
        got = parcel[jnp.maximum(group, 0)].reshape(rows, piece)
        left[:, k * piece : (k + 1) * piece] = jnp.where(group >= 0, got, jnp.zeros_like(got))


Q = 0.5 * DT * DT
G0 = Q * 3.25 * 0.1 * 0.005 * 0.5
G1 = Q * 3.25 * 0.1 * 0.8 * 135.0 * 0.005 * 0.5
G2 = Q * 22.0 * 0.05 * 0.25 * 135.0 * 0.005 * 0.5
DRIVE = Q * 3.25 * 0.1


def increments(y, z, drive):
    steep = (0.28 * 135.0) * y[0]
    t0 = jnp.tanh(0.28 * (y[1] - y[2]) - 1.68)
    t1 = jnp.tanh(steep - 1.68)
    t2 = jnp.tanh(0.25 * steep - 1.68)
    return (
        G0 * t0 + G0 - (Q * 0.2 / DT) * z[0] - (Q * 0.01) * y[0],
        G1 * t1 + drive - (Q * 0.2 / DT) * z[1] - (Q * 0.01) * y[1],
        G2 * t2 + G2 - (Q * 0.1 / DT) * z[2] - (Q * 0.0025) * y[2],
    )


def hold_kernel(after, weights, held, sem):
    load = pltpu.make_async_copy(
        weights.at[pl.ds(0, held.shape[0]), :, pl.ds(0, held.shape[2])], held, sem
    )
    load.start()
    load.wait()


def evolve_kernel(
    own, parcel, held, weights, initial, noise, lead, state, sensors,
    stack, start, rate, gains, left, coupled, potential, sems, out_sems, *, tiles, piece, width
):
    replicas, nodes = noise.shape
    chunks = nodes // width
    early = held.shape[0]
    loads = [
        pltpu.make_async_copy(
            weights.at[pl.ds(first, tiles - first), :, pl.ds(i * width, width)],
            stack.at[i, pl.ds(first, tiles - first)],
            sems.at[i],
        )
        for i in range(chunks)
        for first in [0 if i else early]
    ]
    others = [
        pltpu.make_async_copy(initial, start, sems.at[chunks]),
        pltpu.make_async_copy(noise, rate, sems.at[chunks + 1]),
        pltpu.make_async_copy(lead, gains, sems.at[chunks + 2]),
    ]
    for load in (loads[0], *others, *loads[1:]):
        load.start()
    fill_left(own, parcel, left, tiles, piece)

    def strip(lanes):
        y = [start[r, :, lanes] for r in range(3)]
        z = [DT * start[r, :, lanes] for r in range(3, 6)]
        noisy = DRIVE * rate[:, lanes] + G1
        drives = [
            noisy + (0.5 * DRIVE) * coupled[t * replicas : (t + 1) * replicas, lanes]
            for t in range(2)
        ]
        for s in range(STEPS):
            w = increments(y, z, drives[s])
            y = [a + b for a, b in zip(y, z)]
            part = [a + b for a, b in zip(z, w)]
            second = increments(y, [a + b for a, b in zip(part, w)], drives[s + 1])
            y = [a + b for a, b in zip(y, w)]
            z = [a + b for a, b in zip(part, second)]
            potential[s * replicas : (s + 1) * replicas, lanes] = (y[1] - y[2]).astype(
                potential.dtype
            )
            if s + 2 < TIMES:
                drives.append(
                    noisy
                    + (0.5 * DRIVE) * coupled[(s + 2) * replicas : (s + 3) * replicas, lanes]
                )
        for r in range(3):
            start[r, :, lanes] = y[r]
            start[r + 3, :, lanes] = (1.0 / DT) * z[r]

    stores = []
    def product(first, some):
        depth = some.shape[0] * piece
        return jnp.dot(
            left[:, first * piece : first * piece + depth],
            some.reshape(depth, width),
            preferred_element_type=jnp.float32,
        )

    for i in range(chunks):
        lanes = slice(i * width, (i + 1) * width)
        if i:
            loads[i].wait()
            coupled[:, lanes] = product(0, stack[i])
        else:
            part = product(0, held[...])
            loads[i].wait()
            coupled[:, lanes] = part + product(early, stack[i, early:])
        if i == 0:
            for other in others:
                other.wait()
        strip(lanes)
        stores.append(
            pltpu.make_async_copy(
                start.at[:, :, lanes], state.at[:, :, lanes], out_sems.at[i]
            )
        )
        stores[-1].start()
    local = lax.dot_general(
        potential[...], gains[...], (((1,), (1,)), ((), ())), preferred_element_type=jnp.float32
    )
    sensors[...] = local.reshape(sensors.shape)
    for store in stores:
        store.wait()


def to_all(x, axis):
    copies = jnp.broadcast_to(x, (lax.axis_size(axis), *x.shape))
    return lax.all_to_all(copies, axis, split_axis=0, concat_axis=0, tiled=True)


def total_of(parts):
    mine = jnp.sum(lax.all_to_all(parts, SPREAD, split_axis=0, concat_axis=0, tiled=True), axis=0)
    mine = jnp.sum(to_all(mine, REST), axis=0)
    return to_all(mine, SPREAD)


def body(
    initial, afferent_noise_level, history, weights, lead_field, src_group, src_sub, delays, counts
):
    owners = lax.axis_size(GRP)
    columns = lax.axis_size(NODE)
    my_group = lax.axis_index(GRP)
    my_column = lax.axis_index(NODE)
    myself = my_group * columns + my_column
    cycle, replicas, nodes = history.shape
    tiles, piece = weights.shape[1:3]
    sensors_count = lead_field.shape[0]
    lanes = jnp.arange(tiles, dtype=jnp.int32)

    group_t = src_group.T
    group = my_group.astype(jnp.int32).reshape(1)
    column = my_column.astype(jnp.int32).reshape(1)
    live = lanes[:, None] < counts[None, :]
    mine = (jnp.arange(counts.shape[0], dtype=jnp.int32) == myself)[None, :] & live
    own = jnp.sum(jnp.where(mine, group_t + 1, 0), axis=1) - 1

    smem = pl.BlockSpec(memory_space=pltpu.SMEM)
    vmem = pl.BlockSpec(memory_space=pltpu.VMEM)
    far = pl.BlockSpec(memory_space=pltpu.HBM)
    bf16, f32 = jnp.bfloat16, jnp.float32

    def near(x):
        return pltpu.with_memory_space_constraint(x, pltpu.VMEM)

    def outside(x):
        return pltpu.with_memory_space_constraint(x, pltpu.HBM)


    packed = pl.pallas_call(
        functools.partial(pack_kernel, columns=columns, piece=piece),
        out_shape=pltpu.HBM((owners, TIMES, replicas, piece), bf16),
        in_specs=[smem, smem, far, far, far, far, far, far],
        out_specs=far,
        scratch_shapes=[
            pltpu.VMEM((cycle + 1, replicas, nodes), bf16),
            pltpu.VMEM((owners, TIMES, replicas, piece), bf16),
            pltpu.VMEM((2, replicas, nodes), f32),
            pltpu.VMEM((3, *group_t.shape), jnp.int32),
            pltpu.VMEM((1, counts.shape[0]), jnp.int32),
            pltpu.VMEM((1, counts.shape[0]), jnp.int32),
            pltpu.SMEM((1, counts.shape[0]), jnp.int32),
            pltpu.SemaphoreType.DMA((4,)),
            pltpu.SemaphoreType.DMA((owners,)),
            pltpu.SemaphoreType.DMA,
            pltpu.SemaphoreType.DMA((4,)),
            pltpu.SemaphoreType.DMA,
        ],
        compiler_params=pltpu.CompilerParams(vmem_limit_bytes=16 * MIB),
        name="pack",
    )(
        group,
        column,
        outside(group_t),
        outside(src_sub.T),
        outside(delays.T),
        outside(counts[None, :]),
        outside(history),
        outside(initial),
    )
    parcel = lax.all_to_all(packed, GRP, split_axis=0, concat_axis=0, tiled=True)

    tile_stack = outside(weights.reshape(tiles, piece, nodes))
    width, early = nodes // 2, tiles // 2
    spread = lax.axis_size(SPREAD)
    chunks = nodes // width
    held = pl.pallas_call(
        hold_kernel,
        out_shape=pltpu.VMEM((early, piece, width), bf16),
        in_specs=[far, far],
        out_specs=vmem,
        scratch_shapes=[pltpu.SemaphoreType.DMA],
        compiler_params=pltpu.CompilerParams(vmem_limit_bytes=4 * MIB),
        name="hold",
    )(outside(packed), tile_stack)
    state, local = pl.pallas_call(
        functools.partial(evolve_kernel, tiles=tiles, piece=piece, width=width),
        out_shape=(
            pltpu.HBM(initial.shape, f32),
            pltpu.VMEM((spread, STEPS * replicas // spread, sensors_count), f32),
        ),
        in_specs=[smem, vmem, vmem, far, far, far, far],
        out_specs=(far, vmem),
        scratch_shapes=[
            pltpu.VMEM((chunks, tiles, piece, width), bf16),
            pltpu.VMEM(initial.shape, f32),
            pltpu.VMEM(afferent_noise_level.shape, f32),
            pltpu.VMEM(lead_field.shape, bf16),
            pltpu.VMEM((TIMES * replicas, tiles * piece), bf16),
            pltpu.VMEM((TIMES * replicas, nodes), f32),
            pltpu.VMEM((STEPS * replicas, nodes), bf16),
            pltpu.SemaphoreType.DMA((chunks + 3,)),
            pltpu.SemaphoreType.DMA((chunks,)),
        ],
        compiler_params=pltpu.CompilerParams(vmem_limit_bytes=32 * MIB),
        name="evolve",
    )(
        own,
        near(parcel),
        near(held),
        tile_stack,
        outside(initial),
        outside(afferent_noise_level),
        outside(lead_field),
    )

    total = total_of(local)
    sensors = jnp.transpose(total.reshape(STEPS, replicas, sensors_count), (0, 2, 1))
    return state, sensors


def solution(mesh):
    finer = Mesh(mesh.devices.reshape(2, 2, 8, 4, 2), GRP_NODE)
    placed = (
        P(None, None, GRP_NODE),
        P(None, GRP_NODE),
        P(None, None, GRP_NODE),
        P(GRP_NODE, None, None, None),
        P(None, GRP_NODE),
        P(),
        P(),
        P(),
        P(),
    )
    return jax.shard_map(
        body, mesh=finer, in_specs=placed, out_specs=(P(None, None, GRP_NODE), P()), check_vma=False
    )
```

```python
import functools

import jax
import jax.numpy as jnp
from jax import lax
from jax.experimental import pallas as pl
from jax.experimental.pallas import tpu as pltpu
from jax.sharding import Mesh
from jax.sharding import PartitionSpec as P

STEPS = 6
TIMES = STEPS + 1
GRP = ("grp_0", "grp_1", "grp_2")
NODE = ("node_0", "node_1")
GRP_NODE = GRP + NODE
SPREAD = ("grp_1", "node_0", "node_1")
REST = ("grp_0", "grp_2")

DT = 0.5
MIB = 1 << 20


def firing(v):
    return 1.0 / (1.0 + jnp.exp(0.56 * (6.0 - v)))


def pack_kernel(
    group, column, groups, subs, delays, counts, history, initial, out,
    whole, parts, rows, tables, limits, codes, chosen, gets, puts, row_sem, table_sems, code_sem, *, columns, piece
):
    owners = out.shape[0]
    tiles, blocks = tables.shape[1:]
    cycle = history.shape[0]
    some = cycle // gets.shape[0]
    loads = [
        pltpu.make_async_copy(
            history.at[pl.ds(i * some, some)], whole.at[pl.ds(i * some, some)], gets.at[i]
        )
        for i in range(gets.shape[0])
    ]
    load_rows = pltpu.make_async_copy(initial.at[pl.ds(1, 2)], rows, row_sem)
    lookups = [
        pltpu.make_async_copy(table, tables.at[i], table_sems.at[i])
        for i, table in enumerate((groups, subs, delays))
    ] + [pltpu.make_async_copy(counts, limits, table_sems.at[3])]
    for load in (*lookups, load_rows, *loads):
        load.start()
    for load in lookups:
        load.wait()
    lanes = lax.broadcasted_iota(jnp.int32, (tiles, blocks), 0)
    mine = (tables[0] == group[0]) & (lanes < limits[...])
    code = jnp.sum(jnp.where(mine, (cycle - tables[2]) * 8 + tables[1], 0), axis=0, keepdims=True)
    codes[...] = code
    move = pltpu.make_async_copy(codes, chosen, code_sem)
    move.start()
    load_rows.wait()
    whole[cycle] = firing(rows[0] - rows[1]).astype(whole.dtype)
    move.wait()
    for load in loads:
        load.wait()

    def put(g):
        return pltpu.make_async_copy(parts.at[g], out.at[g], puts.at[g])

    for g in range(owners):
        code = chosen[0, g * columns + column[0]]
        sub = pl.multiple_of((code & 7) * piece, piece)
        parts[g] = whole[pl.ds(code >> 3, TIMES), :, pl.ds(sub, piece)]
        put(g).start()
    for g in range(owners):
        put(g).wait()


def fill_left(own, parcel, left, tiles, piece):
    rows = left.shape[0]
    for k in range(tiles):
        group = own[k]
        got = parcel[jnp.maximum(group, 0)].reshape(rows, piece)
        left[:, k * piece : (k + 1) * piece] = jnp.where(group >= 0, got, jnp.zeros_like(got))


Q = 0.5 * DT * DT
G0 = Q * 3.25 * 0.1 * 0.005 * 0.5
G1 = Q * 3.25 * 0.1 * 0.8 * 135.0 * 0.005 * 0.5
G2 = Q * 22.0 * 0.05 * 0.25 * 135.0 * 0.005 * 0.5
DRIVE = Q * 3.25 * 0.1


def increments(y, z, drive):
    steep = (0.28 * 135.0) * y[0]
    t0 = jnp.tanh(0.28 * (y[1] - y[2]) - 1.68)
    t1 = jnp.tanh(steep - 1.68)
    t2 = jnp.tanh(0.25 * steep - 1.68)
    return (
        G0 * t0 + G0 - (Q * 0.2 / DT) * z[0] - (Q * 0.01) * y[0],
        G1 * t1 + drive - (Q * 0.2 / DT) * z[1] - (Q * 0.01) * y[1],
        G2 * t2 + G2 - (Q * 0.1 / DT) * z[2] - (Q * 0.0025) * y[2],
    )


def hold_kernel(after, weights, held, sem):
    load = pltpu.make_async_copy(
        weights.at[pl.ds(0, held.shape[0]), :, pl.ds(0, held.shape[2])], held, sem
    )
    load.start()
    load.wait()


def evolve_kernel(
    own, parcel, held, weights, initial, noise, lead, state, sensors,
    stack, start, rate, gains, left, coupled, potential, sems, out_sems, *, tiles, piece, width
):
    replicas, nodes = noise.shape
    chunks = nodes // width
    early = held.shape[0]
    loads = [
        pltpu.make_async_copy(
            weights.at[pl.ds(first, tiles - first), :, pl.ds(i * width, width)],
            stack.at[i, pl.ds(first, tiles - first)],
            sems.at[i],
        )
        for i in range(chunks)
        for first in [0 if i else early]
    ]
    others = [
        pltpu.make_async_copy(initial, start, sems.at[chunks]),
        pltpu.make_async_copy(noise, rate, sems.at[chunks + 1]),
        pltpu.make_async_copy(lead, gains, sems.at[chunks + 2]),
    ]
    for load in (loads[0], *others, *loads[1:]):
        load.start()
    fill_left(own, parcel, left, tiles, piece)

    def strip(lanes):
        y = [start[r, :, lanes] for r in range(3)]
        z = [DT * start[r, :, lanes] for r in range(3, 6)]
        noisy = DRIVE * rate[:, lanes] + G1
        drives = [
            noisy + (0.5 * DRIVE) * coupled[t * replicas : (t + 1) * replicas, lanes]
            for t in range(2)
        ]
        for s in range(STEPS):
            w = increments(y, z, drives[s])
            y = [a + b for a, b in zip(y, z)]
            part = [a + b for a, b in zip(z, w)]
            second = increments(y, [a + b for a, b in zip(part, w)], drives[s + 1])
            y = [a + b for a, b in zip(y, w)]
            z = [a + b for a, b in zip(part, second)]
            potential[s * replicas : (s + 1) * replicas, lanes] = (y[1] - y[2]).astype(
                potential.dtype
            )
            if s + 2 < TIMES:
                drives.append(
                    noisy
                    + (0.5 * DRIVE) * coupled[(s + 2) * replicas : (s + 3) * replicas, lanes]
                )
        for r in range(3):
            start[r, :, lanes] = y[r]
            start[r + 3, :, lanes] = (1.0 / DT) * z[r]

    stores = []
    def product(first, some):
        depth = some.shape[0] * piece
        return jnp.dot(
            left[:, first * piece : first * piece + depth],
            some.reshape(depth, width),
            preferred_element_type=jnp.float32,
        )

    for i in range(chunks):
        lanes = slice(i * width, (i + 1) * width)
        if i:
            loads[i].wait()
            coupled[:, lanes] = product(0, stack[i])
        else:
            part = product(0, held[...])
            loads[i].wait()
            coupled[:, lanes] = part + product(early, stack[i, early:])
        if i == 0:
            for other in others:
                other.wait()
        strip(lanes)
        stores.append(
            pltpu.make_async_copy(
                start.at[:, :, lanes], state.at[:, :, lanes], out_sems.at[i]
            )
        )
        stores[-1].start()
    local = lax.dot_general(
        potential[...], gains[...], (((1,), (1,)), ((), ())), preferred_element_type=jnp.float32
    )
    for i in range(sensors.shape[0]):
        for j in range(sensors.shape[1]):
            row = (i * sensors.shape[1] + j) * 4
            sensors[i, j] = local[row : row + 4]
    for store in stores:
        store.wait()


def to_all(x, axis):
    copies = jnp.broadcast_to(x, (lax.axis_size(axis), *x.shape))
    return lax.all_to_all(copies, axis, split_axis=0, concat_axis=0, tiled=True)


def total_of(parts):
    mine = jnp.sum(lax.all_to_all(parts, SPREAD, split_axis=0, concat_axis=0, tiled=True), axis=0)
    mine = jnp.sum(to_all(mine, REST), axis=0)
    return to_all(mine, SPREAD)


def body(
    initial, afferent_noise_level, history, weights, lead_field, src_group, src_sub, delays, counts
):
    owners = lax.axis_size(GRP)
    columns = lax.axis_size(NODE)
    my_group = lax.axis_index(GRP)
    my_column = lax.axis_index(NODE)
    myself = my_group * columns + my_column
    cycle, replicas, nodes = history.shape
    tiles, piece = weights.shape[1:3]
    sensors_count = lead_field.shape[0]
    lanes = jnp.arange(tiles, dtype=jnp.int32)

    group_t = src_group.T
    group = my_group.astype(jnp.int32).reshape(1)
    column = my_column.astype(jnp.int32).reshape(1)
    live = lanes[:, None] < counts[None, :]
    mine = (jnp.arange(counts.shape[0], dtype=jnp.int32) == myself)[None, :] & live
    own = jnp.sum(jnp.where(mine, group_t + 1, 0), axis=1) - 1

    smem = pl.BlockSpec(memory_space=pltpu.SMEM)
    vmem = pl.BlockSpec(memory_space=pltpu.VMEM)
    far = pl.BlockSpec(memory_space=pltpu.HBM)
    bf16, f32 = jnp.bfloat16, jnp.float32

    def near(x):
        return pltpu.with_memory_space_constraint(x, pltpu.VMEM)

    def outside(x):
        return pltpu.with_memory_space_constraint(x, pltpu.HBM)


    packed = pl.pallas_call(
        functools.partial(pack_kernel, columns=columns, piece=piece),
        out_shape=pltpu.HBM((owners, TIMES, replicas, piece), bf16),
        in_specs=[smem, smem, far, far, far, far, far, far],
        out_specs=far,
        scratch_shapes=[
            pltpu.VMEM((cycle + 1, replicas, nodes), bf16),
            pltpu.VMEM((owners, TIMES, replicas, piece), bf16),
            pltpu.VMEM((2, replicas, nodes), f32),
            pltpu.VMEM((3, *group_t.shape), jnp.int32),
            pltpu.VMEM((1, counts.shape[0]), jnp.int32),
            pltpu.VMEM((1, counts.shape[0]), jnp.int32),
            pltpu.SMEM((1, counts.shape[0]), jnp.int32),
            pltpu.SemaphoreType.DMA((4,)),
            pltpu.SemaphoreType.DMA((owners,)),
            pltpu.SemaphoreType.DMA,
            pltpu.SemaphoreType.DMA((4,)),
            pltpu.SemaphoreType.DMA,
        ],
        compiler_params=pltpu.CompilerParams(vmem_limit_bytes=16 * MIB),
        name="pack",
    )(
        group,
        column,
        outside(group_t),
        outside(src_sub.T),
        outside(delays.T),
        outside(counts[None, :]),
        outside(history),
        outside(initial),
    )
    parcel = lax.all_to_all(packed, GRP, split_axis=0, concat_axis=0, tiled=True)

    tile_stack = outside(weights.reshape(tiles, piece, nodes))
    width, early = nodes // 2, tiles // 2
    spread = lax.axis_size(SPREAD)
    chunks = nodes // width
    held = pl.pallas_call(
        hold_kernel,
        out_shape=pltpu.VMEM((early, piece, width), bf16),
        in_specs=[far, far],
        out_specs=vmem,
        scratch_shapes=[pltpu.SemaphoreType.DMA],
        compiler_params=pltpu.CompilerParams(vmem_limit_bytes=4 * MIB),
        name="hold",
    )(outside(packed), tile_stack)
    state, local = pl.pallas_call(
        functools.partial(evolve_kernel, tiles=tiles, piece=piece, width=width),
        out_shape=(
            pltpu.HBM(initial.shape, f32),
            pltpu.VMEM((spread, STEPS * replicas // spread // 4, 4, sensors_count), f32),
        ),
        in_specs=[smem, vmem, vmem, far, far, far, far],
        out_specs=(far, vmem),
        scratch_shapes=[
            pltpu.VMEM((chunks, tiles, piece, width), bf16),
            pltpu.VMEM(initial.shape, f32),
            pltpu.VMEM(afferent_noise_level.shape, f32),
            pltpu.VMEM(lead_field.shape, bf16),
            pltpu.VMEM((TIMES * replicas, tiles * piece), bf16),
            pltpu.VMEM((TIMES * replicas, nodes), f32),
            pltpu.VMEM((STEPS * replicas, nodes), bf16),
            pltpu.SemaphoreType.DMA((chunks + 3,)),
            pltpu.SemaphoreType.DMA((chunks,)),
        ],
        compiler_params=pltpu.CompilerParams(vmem_limit_bytes=32 * MIB),
        name="evolve",
    )(
        own,
        near(parcel),
        near(held),
        tile_stack,
        outside(initial),
        outside(afferent_noise_level),
        outside(lead_field),
    )

    total = total_of(local)
    sensors = jnp.transpose(total.reshape(STEPS, replicas, sensors_count), (0, 2, 1))
    return state, sensors


def solution(mesh):
    finer = Mesh(mesh.devices.reshape(2, 2, 8, 4, 2), GRP_NODE)
    placed = (
        P(None, None, GRP_NODE),
        P(None, GRP_NODE),
        P(None, None, GRP_NODE),
        P(GRP_NODE, None, None, None),
        P(None, GRP_NODE),
        P(),
        P(),
        P(),
        P(),
    )
    return jax.shard_map(
        body, mesh=finer, in_specs=placed, out_specs=(P(None, None, GRP_NODE), P()), check_vma=False
    )
```

```python
import functools

import jax
import jax.numpy as jnp
from jax import lax
from jax.experimental import pallas as pl
from jax.experimental.pallas import tpu as pltpu
from jax.sharding import Mesh
from jax.sharding import PartitionSpec as P

STEPS = 6
TIMES = STEPS + 1
GRP = ("grp_0", "grp_1", "grp_2")
NODE = ("node_0", "node_1")
GRP_NODE = GRP + NODE
SPREAD = ("grp_1", "node_0", "node_1")
REST = ("grp_0", "grp_2")

DT = 0.5
MIB = 1 << 20


def firing(v):
    return 1.0 / (1.0 + jnp.exp(0.56 * (6.0 - v)))


def pack_kernel(
    group, column, groups, subs, delays, counts, history, initial, out,
    whole, parts, rows, tables, limits, codes, chosen, gets, puts, row_sem, table_sems, code_sem, *, columns, piece
):
    owners = out.shape[0]
    tiles, blocks = tables.shape[1:]
    cycle = history.shape[0]
    some = cycle // gets.shape[0]
    loads = [
        pltpu.make_async_copy(
            history.at[pl.ds(i * some, some)], whole.at[pl.ds(i * some, some)], gets.at[i]
        )
        for i in range(gets.shape[0])
    ]
    load_rows = pltpu.make_async_copy(initial.at[pl.ds(1, 2)], rows, row_sem)
    lookups = [
        pltpu.make_async_copy(table, tables.at[i], table_sems.at[i])
        for i, table in enumerate((groups, subs, delays))
    ] + [pltpu.make_async_copy(counts, limits, table_sems.at[3])]
    for load in (*lookups, load_rows, *loads):
        load.start()
    for load in lookups:
        load.wait()
    lanes = lax.broadcasted_iota(jnp.int32, (tiles, blocks), 0)
    mine = (tables[0] == group[0]) & (lanes < limits[...])
    code = jnp.sum(jnp.where(mine, (cycle - tables[2]) * 8 + tables[1], 0), axis=0, keepdims=True)
    codes[...] = code
    move = pltpu.make_async_copy(codes, chosen, code_sem)
    move.start()
    load_rows.wait()
    whole[cycle] = firing(rows[0] - rows[1]).astype(whole.dtype)
    move.wait()
    for load in loads:
        load.wait()

    together = owners // puts.shape[0]

    def put(i):
        some = pl.ds(i * together, together)
        return pltpu.make_async_copy(parts.at[some], out.at[some], puts.at[i])

    for g in range(owners):
        code = chosen[0, g * columns + column[0]]
        sub = pl.multiple_of((code & 7) * piece, piece)
        parts[g] = whole[pl.ds(code >> 3, TIMES), :, pl.ds(sub, piece)]
        if g % together == together - 1:
            put(g // together).start()
    for i in range(puts.shape[0]):
        put(i).wait()


def fill_left(own, parcel, left, tiles, piece):
    rows = left.shape[0]
    for k in range(tiles):
        group = own[k]
        got = parcel[jnp.maximum(group, 0)].reshape(rows, piece)
        left[:, k * piece : (k + 1) * piece] = jnp.where(group >= 0, got, jnp.zeros_like(got))


Q = 0.5 * DT * DT
G0 = Q * 3.25 * 0.1 * 0.005 * 0.5
G1 = Q * 3.25 * 0.1 * 0.8 * 135.0 * 0.005 * 0.5
G2 = Q * 22.0 * 0.05 * 0.25 * 135.0 * 0.005 * 0.5
DRIVE = Q * 3.25 * 0.1


def increments(y, z, drive):
    steep = (0.28 * 135.0) * y[0]
    t0 = jnp.tanh(0.28 * (y[1] - y[2]) - 1.68)
    t1 = jnp.tanh(steep - 1.68)
    t2 = jnp.tanh(0.25 * steep - 1.68)
    return (
        G0 * t0 + G0 - (Q * 0.2 / DT) * z[0] - (Q * 0.01) * y[0],
        G1 * t1 + drive - (Q * 0.2 / DT) * z[1] - (Q * 0.01) * y[1],
        G2 * t2 + G2 - (Q * 0.1 / DT) * z[2] - (Q * 0.0025) * y[2],
    )


def hold_kernel(after, weights, held, sem):
    load = pltpu.make_async_copy(
        weights.at[pl.ds(0, held.shape[0]), :, pl.ds(0, held.shape[2])], held, sem
    )
    load.start()
    load.wait()


def evolve_kernel(
    own, parcel, held, weights, initial, noise, lead, state, sensors,
    stack, start, rate, gains, left, coupled, potential, sems, out_sems, *, tiles, piece, width
):
    replicas, nodes = noise.shape
    chunks = nodes // width
    early = held.shape[0]
    loads = [
        pltpu.make_async_copy(
            weights.at[pl.ds(first, tiles - first), :, pl.ds(i * width, width)],
            stack.at[i, pl.ds(first, tiles - first)],
            sems.at[i],
        )
        for i in range(chunks)
        for first in [0 if i else early]
    ]
    others = [
        pltpu.make_async_copy(initial, start, sems.at[chunks]),
        pltpu.make_async_copy(noise, rate, sems.at[chunks + 1]),
        pltpu.make_async_copy(lead, gains, sems.at[chunks + 2]),
    ]
    for load in (loads[0], *others, *loads[1:]):
        load.start()
    fill_left(own, parcel, left, tiles, piece)

    def strip(lanes):
        y = [start[r, :, lanes] for r in range(3)]
        z = [DT * start[r, :, lanes] for r in range(3, 6)]
        noisy = DRIVE * rate[:, lanes] + G1
        drives = [
            noisy + (0.5 * DRIVE) * coupled[t * replicas : (t + 1) * replicas, lanes]
            for t in range(2)
        ]
        for s in range(STEPS):
            w = increments(y, z, drives[s])
            y = [a + b for a, b in zip(y, z)]
            part = [a + b for a, b in zip(z, w)]
            second = increments(y, [a + b for a, b in zip(part, w)], drives[s + 1])
            y = [a + b for a, b in zip(y, w)]
            z = [a + b for a, b in zip(part, second)]
            potential[s * replicas : (s + 1) * replicas, lanes] = (y[1] - y[2]).astype(
                potential.dtype
            )
            if s + 2 < TIMES:
                drives.append(
                    noisy
                    + (0.5 * DRIVE) * coupled[(s + 2) * replicas : (s + 3) * replicas, lanes]
                )
        for r in range(3):
            start[r, :, lanes] = y[r]
            start[r + 3, :, lanes] = (1.0 / DT) * z[r]

    stores = []
    def product(first, some):
        depth = some.shape[0] * piece
        return jnp.dot(
            left[:, first * piece : first * piece + depth],
            some.reshape(depth, width),
            preferred_element_type=jnp.float32,
        )

    for i in range(chunks):
        lanes = slice(i * width, (i + 1) * width)
        if i:
            loads[i].wait()
            coupled[:, lanes] = product(0, stack[i])
        else:
            part = product(0, held[...])
            loads[i].wait()
            coupled[:, lanes] = part + product(early, stack[i, early:])
        if i == 0:
            for other in others:
                other.wait()
        strip(lanes)
        stores.append(
            pltpu.make_async_copy(
                start.at[:, :, lanes], state.at[:, :, lanes], out_sems.at[i]
            )
        )
        stores[-1].start()
    local = lax.dot_general(
        potential[...], gains[...], (((1,), (1,)), ((), ())), preferred_element_type=jnp.float32
    )
    for i in range(sensors.shape[0]):
        for j in range(sensors.shape[1]):
            row = (i * sensors.shape[1] + j) * 4
            sensors[i, j] = local[row : row + 4]
    for store in stores:
        store.wait()


def to_all(x, axis):
    copies = jnp.broadcast_to(x, (lax.axis_size(axis), *x.shape))
    return lax.all_to_all(copies, axis, split_axis=0, concat_axis=0, tiled=True)


def total_of(parts):
    mine = jnp.sum(lax.all_to_all(parts, SPREAD, split_axis=0, concat_axis=0, tiled=True), axis=0)
    mine = jnp.sum(to_all(mine, REST), axis=0)
    return to_all(mine, SPREAD)


def body(
    initial, afferent_noise_level, history, weights, lead_field, src_group, src_sub, delays, counts
):
    owners = lax.axis_size(GRP)
    columns = lax.axis_size(NODE)
    my_group = lax.axis_index(GRP)
    my_column = lax.axis_index(NODE)
    myself = my_group * columns + my_column
    cycle, replicas, nodes = history.shape
    tiles, piece = weights.shape[1:3]
    sensors_count = lead_field.shape[0]
    lanes = jnp.arange(tiles, dtype=jnp.int32)

    group_t = src_group.T
    group = my_group.astype(jnp.int32).reshape(1)
    column = my_column.astype(jnp.int32).reshape(1)
    live = lanes[:, None] < counts[None, :]
    mine = (jnp.arange(counts.shape[0], dtype=jnp.int32) == myself)[None, :] & live
    own = jnp.sum(jnp.where(mine, group_t + 1, 0), axis=1) - 1

    smem = pl.BlockSpec(memory_space=pltpu.SMEM)
    vmem = pl.BlockSpec(memory_space=pltpu.VMEM)
    far = pl.BlockSpec(memory_space=pltpu.HBM)
    bf16, f32 = jnp.bfloat16, jnp.float32

    def near(x):
        return pltpu.with_memory_space_constraint(x, pltpu.VMEM)

    def outside(x):
        return pltpu.with_memory_space_constraint(x, pltpu.HBM)


    packed = pl.pallas_call(
        functools.partial(pack_kernel, columns=columns, piece=piece),
        out_shape=pltpu.HBM((owners, TIMES, replicas, piece), bf16),
        in_specs=[smem, smem, far, far, far, far, far, far],
        out_specs=far,
        scratch_shapes=[
            pltpu.VMEM((cycle + 1, replicas, nodes), bf16),
            pltpu.VMEM((owners, TIMES, replicas, piece), bf16),
            pltpu.VMEM((2, replicas, nodes), f32),
            pltpu.VMEM((3, *group_t.shape), jnp.int32),
            pltpu.VMEM((1, counts.shape[0]), jnp.int32),
            pltpu.VMEM((1, counts.shape[0]), jnp.int32),
            pltpu.SMEM((1, counts.shape[0]), jnp.int32),
            pltpu.SemaphoreType.DMA((8,)),
            pltpu.SemaphoreType.DMA((8,)),
            pltpu.SemaphoreType.DMA,
            pltpu.SemaphoreType.DMA((4,)),
            pltpu.SemaphoreType.DMA,
        ],
        compiler_params=pltpu.CompilerParams(vmem_limit_bytes=16 * MIB),
        name="pack",
    )(
        group,
        column,
        outside(group_t),
        outside(src_sub.T),
        outside(delays.T),
        outside(counts[None, :]),
        outside(history),
        outside(initial),
    )
    parcel = lax.all_to_all(packed, GRP, split_axis=0, concat_axis=0, tiled=True)

    tile_stack = outside(weights.reshape(tiles, piece, nodes))
    width, early = nodes // 2, tiles // 2
    spread = lax.axis_size(SPREAD)
    chunks = nodes // width
    held = pl.pallas_call(
        hold_kernel,
        out_shape=pltpu.VMEM((early, piece, width), bf16),
        in_specs=[far, far],
        out_specs=vmem,
        scratch_shapes=[pltpu.SemaphoreType.DMA],
        compiler_params=pltpu.CompilerParams(vmem_limit_bytes=4 * MIB),
        name="hold",
    )(outside(packed), tile_stack)
    state, local = pl.pallas_call(
        functools.partial(evolve_kernel, tiles=tiles, piece=piece, width=width),
        out_shape=(
            pltpu.HBM(initial.shape, f32),
            pltpu.VMEM((spread, STEPS * replicas // spread // 4, 4, sensors_count), f32),
        ),
        in_specs=[smem, vmem, vmem, far, far, far, far],
        out_specs=(far, vmem),
        scratch_shapes=[
            pltpu.VMEM((chunks, tiles, piece, width), bf16),
            pltpu.VMEM(initial.shape, f32),
            pltpu.VMEM(afferent_noise_level.shape, f32),
            pltpu.VMEM(lead_field.shape, bf16),
            pltpu.VMEM((TIMES * replicas, tiles * piece), bf16),
            pltpu.VMEM((TIMES * replicas, nodes), f32),
            pltpu.VMEM((STEPS * replicas, nodes), bf16),
            pltpu.SemaphoreType.DMA((chunks + 3,)),
            pltpu.SemaphoreType.DMA((chunks,)),
        ],
        compiler_params=pltpu.CompilerParams(vmem_limit_bytes=32 * MIB),
        name="evolve",
    )(
        own,
        near(parcel),
        near(held),
        tile_stack,
        outside(initial),
        outside(afferent_noise_level),
        outside(lead_field),
    )

    total = total_of(local)
    sensors = jnp.transpose(total.reshape(STEPS, replicas, sensors_count), (0, 2, 1))
    return state, sensors


def solution(mesh):
    finer = Mesh(mesh.devices.reshape(2, 2, 8, 4, 2), GRP_NODE)
    placed = (
        P(None, None, GRP_NODE),
        P(None, GRP_NODE),
        P(None, None, GRP_NODE),
        P(GRP_NODE, None, None, None),
        P(None, GRP_NODE),
        P(),
        P(),
        P(),
        P(),
    )
    return jax.shard_map(
        body, mesh=finer, in_specs=placed, out_specs=(P(None, None, GRP_NODE), P()), check_vma=False
    )
```
